128 devices in a mesh: owner: 4 (over x_lo, core), rows: 32 (over z, y, x_hi).
Axes of the slice: x: 4 (x_hi: 2, x_lo: 2; x = x_hi * 2 + x_lo), y: 4, z: 4, core: 2. Of those that a mesh axis runs over, the one named last changes fastest.
Arguments:
- master_down: float32 [8, 14336, 4096], P('owner', None, 'rows'), may hold values from -0.046875 to 0.046875
- router_weight: float32 [4096, 8], P('rows', 'owner'), may hold values from -0.09375 to 0.09375
- router_gain: float32 [4096], P('rows'), may hold values from 0.25 to 1.75
Outputs:
- final_down: bfloat16 [8, 4096, 14336], P('owner', None, 'rows')
- serve_router: bfloat16 [4096, 8], replicated
The draws below stay inside these ranges and needn't reach their ends.
All inputs are finite; a program needn't handle non-finite values.
Results may differ from the reference program's by a relative error of at most 0.001.
Values may be sent and summed in bfloat16 or wider, within the bound.
A program may use at most 128 MiB of HBM per device.

```python
import jax
import jax.numpy as jnp

EXPERTS = 8
D_MODEL = 4096
D_EXPERT = 14336


def steps_of(key, extent, split, smallest, largest):
    def one(axis_at, parts):
        heights = jax.random.uniform(jax.random.fold_in(jax.random.fold_in(key, 6), axis_at), (parts,), jnp.float32, smallest / len(split), largest / len(split))
        return jnp.repeat(jnp.exp(heights), extent[axis_at] // parts).reshape((-1,) + (1,) * (len(extent) - axis_at - 1))

    gain = one(*split[0])
    for cut in split[1:]:
        gain = gain * one(*cut)
    return gain


def noise(own_key, dims, width, reach, pieces=(), dtype=jnp.bfloat16):
    level = steps_of(own_key, dims, pieces, -0.22, 0.18) if pieces else 1.0
    result = jax.random.normal(own_key, dims, jnp.float32) * width * level
    return jnp.minimum(jnp.maximum(result, -reach), reach).astype(dtype)


def setup_inputs(seed: int = 0) -> dict:
    streams_of = jax.random.split(jax.random.key(seed), 4)
    master_down = noise(streams_of[0], (EXPERTS, D_EXPERT, D_MODEL), D_EXPERT ** -0.5, 0.046875, ((0, 4), (2, 32)), jnp.float32)
    router_weight = noise(streams_of[1], (D_MODEL, EXPERTS), D_MODEL ** -0.5, 0.09375, ((0, 32), (1, 4)), jnp.float32)
    router_gain = jnp.clip(1.0 + 0.15 * jax.random.normal(streams_of[2], (D_MODEL,), jnp.float32), 0.25, 1.75)
    return dict(master_down=master_down, router_weight=router_weight, router_gain=router_gain)


def reference(master_down, router_weight, router_gain):
    final_down = master_down.astype(jnp.bfloat16)
    final_down = jnp.transpose(final_down, (0, 2, 1))
    serve_router = (router_weight * router_gain[:, None]).astype(jnp.bfloat16)
    return final_down, serve_router
```

```python
import functools
import itertools

import jax
import jax.numpy as jnp
from jax import lax
from jax.experimental import pallas as pl
from jax.experimental.pallas import tpu as pltpu
from jax.sharding import PartitionSpec as P

MESH = pl.DeviceIdType.MESH
SIZES = (4, 4, 2)
ORDERS = ((0, 1, 2), (1, 2, 0), (2, 0, 1))
OWNERS = 4


def cuts_of(length, count, step):
    tiles = length // step
    edges = [tiles * k // count * step for k in range(count)] + [length]
    return [(a, b - a) for a, b in zip(edges, edges[1:])]


def flat(delta):
    index = 0
    for d, size in zip(delta, SIZES):
        index = index * size + d
    return index


DELTAS = sorted(
    itertools.product(*(range(s) for s in SIZES)),
    key=lambda d: (sum(k == 0 for k in d), d[0] == 2, d[1] == 2, d),
)
OTHERS = [d for d in DELTAS if any(d)]


def travelled(color, phase, delta):
    return [q for q in range(phase) if delta[ORDERS[color][q]]]


def is_final(color, phase, delta):
    return not any(delta[ORDERS[color][q]] for q in range(phase + 1, 3))


def kernel(rows_axis, owner_axis, cuts, x_ref, w_ref, g_ref, out_ref, router_ref, loaded, held, first, second,
           parts, grid, load_sem, send_sem, recv_sem, part_send, part_recv, grid_send, grid_recv):
    me = lax.axis_index(rows_axis)
    own = lax.axis_index(owner_axis)
    place = (me // 8, (me // 2) % 4, me % 2)
    depth = held.shape[2]
    width = held.shape[3]
    relays = (first, second)

    def index_at(coords):
        return (coords[0] * SIZES[1] + coords[1]) * SIZES[2] + coords[2]

    def moved(delta, sign=1):
        return index_at([lax.rem(p + sign * d + s, s) if d else p for p, d, s in zip(place, delta, SIZES)])

    def along(dim, step):
        return moved([step if k == dim else 0 for k in range(3)])

    peers = {(d, k): along(d, k) for d in range(3) for k in range(1, SIZES[d])}
    mates = [lax.rem(own + k, OWNERS) for k in range(OWNERS)]

    barrier = pltpu.get_barrier_semaphore()
    for peer in peers.values():
        pl.semaphore_signal(barrier, inc=1, device_id=(own, peer), device_id_type=MESH)
    for k in range(1, OWNERS):
        pl.semaphore_signal(barrier, inc=1, device_id=(mates[k], me), device_id_type=MESH)

    def load(delta):
        i = flat(delta)
        start = pl.multiple_of(moved(delta) * depth, 8)
        return pltpu.make_async_copy(x_ref.at[:, pl.ds(start, depth), :], loaded.at[i], load_sem.at[i])

    for delta in DELTAS:
        load(delta).start()

    def copy(color, phase, delta):
        i = flat(delta)
        start, size = cuts[color]
        rows = pl.ds(start, size)
        before = travelled(color, phase, delta)
        source = (relays[before[-1]] if before else held).at[i, :, rows, :]
        dim = ORDERS[color][phase]
        if is_final(color, phase, delta):
            gone = [0, 0, 0]
            for q in before:
                gone[ORDERS[color][q]] = delta[ORDERS[color][q]]
            column = pl.multiple_of(moved(gone, -1) * width, 128)
            target = out_ref.at[:, rows, pl.ds(column, width)]
        else:
            target = relays[phase].at[i, :, rows, :]
        return pltpu.make_async_remote_copy(
            src_ref=source, dst_ref=target, send_sem=send_sem.at[color, phase, i], recv_sem=recv_sem.at[color, phase, i],
            device_id=(own, peers[dim, delta[dim]]), device_id_type=MESH)

    def goes(color, phase, delta):
        return delta[ORDERS[color][phase]] != 0

    scaled = (w_ref[...] * g_ref[...]).astype(jnp.bfloat16).astype(jnp.float32)
    line = lax.broadcasted_iota(jnp.int32, (8, width), 0)
    pair = jnp.where(line % 2 == 0, jnp.broadcast_to(scaled[0:1, :], (8, width)), jnp.broadcast_to(scaled[1:2, :], (8, width)))
    parts[0] = pair.astype(jnp.bfloat16)

    def part_copy(k):
        return pltpu.make_async_remote_copy(
            src_ref=parts.at[0], dst_ref=parts.at[k], send_sem=part_send.at[k], recv_sem=part_recv.at[k],
            device_id=(mates[k], me), device_id_type=MESH)

    def grid_copies(dim):
        if dim == 0:
            block = grid.at[place[0], place[1], place[2]]
        elif dim == 1:
            block = grid.at[:, place[1], place[2]]
        else:
            block = grid.at[:, :, place[2]]
        return [
            pltpu.make_async_remote_copy(
                src_ref=block, dst_ref=block, send_sem=grid_send.at[dim, k], recv_sem=grid_recv.at[dim, k],
                device_id=(own, peers[dim, k]), device_id_type=MESH)
            for k in range(1, SIZES[dim])
        ]

    pl.semaphore_wait(barrier, len(peers) + OWNERS - 1)

    waiting = None
    for delta in DELTAS:
        load(delta).wait()
        if any(delta):
            held[flat(delta)] = loaded[flat(delta)].astype(jnp.bfloat16)
        else:
            out_ref[:, :, pl.ds(pl.multiple_of(me * width, 128), width)] = loaded[flat(delta)].astype(jnp.bfloat16)
        if waiting is not None:
            for color in range(3):
                if goes(color, 0, waiting):
                    copy(color, 0, waiting).start()
        waiting = delta if any(delta) else None
    for k in range(1, OWNERS):
        part_copy(k).start()

    for delta in OTHERS:
        for color in range(3):
            if goes(color, 1, delta) and not travelled(color, 1, delta):
                copy(color, 1, delta).start()

    for k in range(1, OWNERS):
        part_copy(k).wait()
    tile = parts[0].astype(jnp.float32)
    for k in range(1, OWNERS):
        theirs = lax.rem(own - k + OWNERS, OWNERS)
        tile = jnp.where(line // 2 == theirs, parts[k].astype(jnp.float32), tile)
    grid[place[0], place[1], place[2]] = tile.astype(jnp.bfloat16)

    count = 0
    for delta in OTHERS:
        for color in range(3):
            if goes(color, 0, delta) and not is_final(color, 0, delta):
                copy(color, 0, delta).wait_recv()
                if goes(color, 1, delta):
                    copy(color, 1, delta).start()
                count += 1
                if count == 4:
                    for c in grid_copies(0):
                        c.start()
                if count == 24:
                    for c in grid_copies(0):
                        c.wait()
                    for c in grid_copies(1):
                        c.start()
                if count == 48:
                    for c in grid_copies(1):
                        c.wait()
                    for c in grid_copies(2):
                        c.start()

    for late in ([], [0]):
        for delta in OTHERS:
            for color in range(3):
                if goes(color, 2, delta) and travelled(color, 2, delta) == late:
                    copy(color, 2, delta).start()
    for c in grid_copies(2):
        c.wait()
    for late in ([1], [0, 1]):
        for delta in OTHERS:
            for color in range(3):
                if goes(color, 2, delta) and travelled(color, 2, delta) == late:
                    copy(color, 1, delta).wait_recv()
                    copy(color, 2, delta).start()
    for row in range(32):
        router_ref[:, row * width : (row + 1) * width] = grid[row // 8, (row // 2) % 4, row % 2]

    for phase in range(3):
        for delta in OTHERS:
            for color in range(3):
                if goes(color, phase, delta):
                    if is_final(color, phase, delta):
                        copy(color, phase, delta).wait_recv()
                    copy(color, phase, delta).wait_send()


def solution(mesh):
    def shards(master_down, router_weight, router_gain):
        experts, long, width = master_down.shape
        n = mesh.shape["rows"]
        depth = long // n
        cuts = cuts_of(depth, 3, 8)
        block = (n, experts, depth, width)
        dma = pltpu.SemaphoreType.DMA
        final, router = pl.pallas_call(
            functools.partial(kernel, "rows", "owner", cuts),
            out_shape=(
                pltpu.VMEM((experts, depth, n * width), jnp.bfloat16),
                pltpu.VMEM((experts * OWNERS, n * width), jnp.bfloat16),
            ),
            in_specs=[
                pl.BlockSpec(memory_space=pl.ANY),
                pl.BlockSpec(memory_space=pltpu.VMEM),
                pl.BlockSpec(memory_space=pltpu.VMEM),
            ],
            out_specs=(pl.BlockSpec(memory_space=pltpu.VMEM), pl.BlockSpec(memory_space=pltpu.VMEM)),
            scratch_shapes=[
                pltpu.VMEM(block, jnp.float32),
                pltpu.VMEM(block, jnp.bfloat16),
                pltpu.VMEM(block, jnp.bfloat16),
                pltpu.VMEM(block, jnp.bfloat16),
                pltpu.VMEM((OWNERS, 8, width), jnp.bfloat16),
                pltpu.VMEM((*SIZES, 8, width), jnp.bfloat16),
                dma((n,)),
                dma((3, 3, n)),
                dma((3, 3, n)),
                dma((OWNERS,)),
                dma((OWNERS,)),
                dma((3, 4)),
                dma((3, 4)),
            ],
            compiler_params=pltpu.CompilerParams(
                collective_id=0, has_side_effects=True, vmem_limit_bytes=48 * 2**20
            ),
        )(master_down, router_weight.T, router_gain.reshape(1, width))
        return jnp.swapaxes(final, 1, 2), router.T

    return jax.shard_map(
        shards,
        mesh=mesh,
        in_specs=(P("owner", None, "rows"), P("rows", "owner"), P("rows")),
        out_specs=(P("owner", None, "rows"), P()),
        check_vma=False,
    )
```

```python
import functools
import itertools

import jax
import jax.numpy as jnp
from jax import lax
from jax.experimental import pallas as pl
from jax.experimental.pallas import tpu as pltpu
from jax.sharding import PartitionSpec as P

MESH = pl.DeviceIdType.MESH
SIZES = (4, 4, 2)
ORDERS = ((0, 1, 2), (1, 2, 0), (2, 0, 1))
COLORS = range(3)
OWNERS = 4
STEPS = {2: (1,), 4: (1, 3, 2)}


def cuts_of(length, count, step):
    tiles = length // step
    edges = [tiles * k // count * step for k in range(count)] + [length]
    return [(a, b - a) for a, b in zip(edges, edges[1:])]


class Move:
    def __init__(self, color, phase, box):
        self.color, self.phase = color, phase
        self.box = tuple(box[k] for k in range(3))
        self.dim = ORDERS[color][phase]
        self.step = self.box[self.dim][0]
        self.index = None

    def deltas(self):
        return list(itertools.product(*(range(a, a + n) for a, n in self.box)))

    def origin(self):
        found = {
            max((q for q in range(self.phase) if d[ORDERS[self.color][q]]), default=None, key=lambda q: q)
            for d in self.deltas()
        }
        (phase,) = found
        return phase


def plan():
    def move(color, phase, a, b, c):
        dims = ORDERS[color]
        return Move(color, phase, {dims[0]: a, dims[1]: b, dims[2]: c})

    def sizes(color):
        return [SIZES[d] for d in ORDERS[color]]

    rest, zero = lambda n: (1, n - 1), (0, 1)
    first, second, third = [], [], []
    for color in COLORS:
        na, nb, nc = sizes(color)
        starts, ends = [], []
        for a in STEPS[na]:
            bs = [rest(nb)] if na == 4 else [(b, 1) for b in STEPS[nb]]
            starts += [move(color, 0, (a, 1), b, (0, nc)) for b in bs]
            ends.append(move(color, 0, (a, 1), zero, (0, nc)))
        first.append(starts + ends)
        second.append(
            [[move(color, 1, zero, (b, 1), (0, nc)) for b in STEPS[nb]]]
            + [[move(color, 1, (a, 1), (b, 1), (0, nc)) for b in STEPS[nb]] for a in STEPS[na]]
        )
        third.append(
            [[move(color, 2, zero, zero, (c, 1)) for c in STEPS[nc]]]
            + [[move(color, 2, rest(na), zero, (c, 1)) for c in STEPS[nc]]]
            + [[move(color, 2, (0, na), (b, 1), (c, 1)) for c in STEPS[nc]] for b in STEPS[nb]]
        )

    def woven(lists):
        return [m for row in itertools.zip_longest(*lists) for m in row if m is not None]

    def woven_rows(lists):
        return [m for row in itertools.zip_longest(*lists) for part in row if part for m in woven([part])]

    stages = (
        woven(first),
        woven([rows[0] for rows in second]),
        woven_rows([rows[1:] for rows in second]),
        woven([rows[0] + rows[1] for rows in third]),
        woven_rows([rows[2:] for rows in third]),
    )
    for k, m in enumerate(itertools.chain(*stages)):
        m.index = k
    return stages


STAGES = plan()
MOVES = list(itertools.chain(*STAGES))
BROUGHT = {(m.color, m.phase, d): m for m in MOVES for d in m.deltas()}
HEAD = 8


def kernel(cuts, x_ref, w_ref, g_ref, out_ref, router_ref, *scratch):
    loaded, held, *relays = (scratch[3 * k : 3 * k + 3] for k in range(5))
    parts, grid, load_sem, send_sem, recv_sem, part_send, part_recv, grid_send, grid_recv = scratch[15:]
    me = lax.axis_index("rows")
    own = lax.axis_index("owner")
    place = (me // 8, (me // 2) % 4, me % 2)
    depth = out_ref.shape[1]
    width = w_ref.shape[1]

    def moved(delta, sign=1):
        z, y, x = (lax.rem(p + sign * d + s, s) if d else p for p, d, s in zip(place, delta, SIZES))
        return (z * SIZES[1] + y) * SIZES[2] + x

    peers = {
        (dim, k): moved([k if d == dim else 0 for d in range(3)]) for dim in range(3) for k in range(1, SIZES[dim])
    }
    mates = [lax.rem(own + k, OWNERS) for k in range(OWNERS)]

    barrier = pltpu.get_barrier_semaphore()
    for peer in peers.values():
        pl.semaphore_signal(barrier, inc=1, device_id=(own, peer), device_id_type=MESH)
    for k in range(1, OWNERS):
        pl.semaphore_signal(barrier, inc=1, device_id=(mates[k], me), device_id_type=MESH)

    def load(color, delta):
        start, size = cuts[color]
        top = pl.multiple_of(moved(delta) * depth + start, 8)
        flat = (delta[0] * SIZES[1] + delta[1]) * SIZES[2] + delta[2]
        return pltpu.make_async_copy(
            x_ref.at[:, pl.ds(top, size), :], loaded[color].at[delta], load_sem.at[color, flat]
        )

    own_moves = [m for m in MOVES if m.origin() is None]
    here = (0, 0, 0)
    for m in own_moves:
        for delta in m.deltas():
            load(m.color, delta).start()
    for color in COLORS:
        load(color, here).start()

    def column(delta):
        return pl.ds(pl.multiple_of(moved(delta, -1) * width, 128), width)

    def cast(m):
        for delta in m.deltas():
            load(m.color, delta).wait()
            held[m.color][delta] = loaded[m.color][delta].astype(jnp.bfloat16)

    def copy(m):
        origin = m.origin()
        box = tuple(pl.ds(a, n) for a, n in m.box)
        source = held if origin is None else relays[origin]
        return pltpu.make_async_remote_copy(
            src_ref=source[m.color].at[box],
            dst_ref=relays[m.phase][m.color].at[box],
            send_sem=send_sem.at[m.index],
            recv_sem=recv_sem.at[m.index],
            device_id=(own, peers[m.dim, m.step]),
            device_id_type=MESH,
        )

    arrived = set()

    def await_arrival(m):
        if m.index in arrived:
            return
        arrived.add(m.index)
        copy(m).wait_recv()
        ended.extend((m, d) for d in m.deltas() if not any(d[ORDERS[m.color][q]] for q in range(m.phase + 1, 3)))

    ended = []

    def settle():
        for m, delta in ended:
            start, size = cuts[m.color]
            out_ref[:, pl.ds(start, size), column(delta)] = relays[m.phase][m.color][delta]
        ended.clear()

    def needs(m):
        origin = m.origin()
        if origin is None:
            return []
        wanted = {BROUGHT[m.color, origin, d].index for d in m.deltas()}
        return [MOVES[k] for k in sorted(wanted)]

    scaled = (w_ref[...] * g_ref[...]).astype(jnp.bfloat16).astype(jnp.float32)
    line = lax.broadcasted_iota(jnp.int32, (8, width), 0)
    pair = jnp.where(
        line % 2 == 0, jnp.broadcast_to(scaled[0:1, :], (8, width)), jnp.broadcast_to(scaled[1:2, :], (8, width))
    )
    parts[0] = pair.astype(jnp.bfloat16)

    def part_copy(k):
        return pltpu.make_async_remote_copy(
            src_ref=parts.at[0], dst_ref=parts.at[k], send_sem=part_send.at[k], recv_sem=part_recv.at[k],
            device_id=(mates[k], me), device_id_type=MESH)

    def grid_copies(dim):
        if dim == 0:
            block = grid.at[place[0], place[1], place[2]]
        elif dim == 1:
            block = grid.at[:, place[1], place[2]]
        else:
            block = grid.at[:, :, place[2]]
        return [
            pltpu.make_async_remote_copy(
                src_ref=block, dst_ref=block, send_sem=grid_send.at[dim, k], recv_sem=grid_recv.at[dim, k],
                device_id=(own, peers[dim, k]), device_id_type=MESH)
            for k in range(1, SIZES[dim])
        ]

    starts = STAGES[0]
    for m in starts[:HEAD]:
        cast(m)
    pl.semaphore_wait(barrier, len(peers) + OWNERS - 1)
    for k in range(1, OWNERS):
        part_copy(k).start()
    for m in starts[:HEAD]:
        copy(m).start()
    previous = None
    for m in starts[HEAD:]:
        cast(m)
        if previous is not None:
            copy(previous).start()
        previous = m
    for k in range(1, OWNERS):
        part_copy(k).wait()
    tile = parts[0].astype(jnp.float32)
    for k in range(1, OWNERS):
        theirs = lax.rem(own - k + OWNERS, OWNERS)
        tile = jnp.where(line // 2 == theirs, parts[k].astype(jnp.float32), tile)
    grid[place[0], place[1], place[2]] = tile.astype(jnp.bfloat16)
    for m in STAGES[1]:
        cast(m)
        if previous is not None:
            copy(previous).start()
        previous = m
    for c in grid_copies(0):
        c.start()
    for m in STAGES[3]:
        if m.origin() is None:
            cast(m)
    copy(previous).start()
    for color in COLORS:
        start, size = cuts[color]
        load(color, here).wait()
        out_ref[:, pl.ds(start, size), column(here)] = loaded[color][here].astype(jnp.bfloat16)

    half = len(STAGES[2]) // 2
    for k, m in enumerate(STAGES[2]):
        for n in needs(m):
            await_arrival(n)
        copy(m).start()
        if k == half:
            for c in grid_copies(0):
                c.wait()
            for c in grid_copies(1):
                c.start()
    for m in STAGES[3]:
        for n in needs(m):
            await_arrival(n)
        copy(m).start()
    for m in starts:
        await_arrival(m)
    settle()
    late = len(STAGES[4]) - 3
    for k, m in enumerate(STAGES[4]):
        for n in needs(m):
            await_arrival(n)
        copy(m).start()
        if k == 0:
            for c in grid_copies(1):
                c.wait()
            for c in grid_copies(2):
                c.start()
    settle()
    for m in MOVES[: len(STAGES[0]) + len(STAGES[1]) + len(STAGES[2])]:
        copy(m).wait_send()
    for c in grid_copies(2):
        c.wait()
    for row in range(32):
        router_ref[:, row * width : (row + 1) * width] = grid[row // 8, (row // 2) % 4, row % 2]
    for m in STAGES[3] + STAGES[4]:
        await_arrival(m)
        settle()
    for m in STAGES[3] + STAGES[4]:
        copy(m).wait_send()


def drain(final_ref, router_ref, final_out, router_out, sems):
    pieces = 8
    height = final_ref.shape[1] // pieces
    copies = [
        pltpu.make_async_copy(
            final_ref.at[e, pl.ds(k * height, height)], final_out.at[e, pl.ds(k * height, height)], sems.at[e * pieces + k]
        )
        for e in range(final_ref.shape[0])
        for k in range(pieces)
    ]
    copies.append(pltpu.make_async_copy(router_ref, router_out, sems.at[len(copies)]))
    for c in copies:
        c.start()
    for c in copies:
        c.wait()


def solution(mesh):
    def shards(master_down, router_weight, router_gain):
        experts, long, width = master_down.shape
        n = mesh.shape["rows"]
        depth = long // n
        cuts = cuts_of(depth, 3, 16)
        dma = pltpu.SemaphoreType.DMA
        blocks = [(*SIZES, experts, size, width) for _, size in cuts]
        final, router = pl.pallas_call(
            functools.partial(kernel, cuts),
            out_shape=(
                pltpu.VMEM((experts, depth, n * width), jnp.bfloat16),
                pltpu.VMEM((experts * OWNERS, n * width), jnp.bfloat16),
            ),
            in_specs=[
                pl.BlockSpec(memory_space=pl.ANY),
                pl.BlockSpec(memory_space=pltpu.VMEM),
                pl.BlockSpec(memory_space=pltpu.VMEM),
            ],
            out_specs=(pl.BlockSpec(memory_space=pltpu.VMEM), pl.BlockSpec(memory_space=pltpu.VMEM)),
            scratch_shapes=[pltpu.VMEM(b, jnp.float32) for b in blocks]
            + [pltpu.VMEM(b, jnp.bfloat16) for _ in range(4) for b in blocks]
            + [
                pltpu.VMEM((OWNERS, 8, width), jnp.bfloat16),
                pltpu.VMEM((*SIZES, 8, width), jnp.bfloat16),
                dma((3, n)),
                dma((len(MOVES),)),
                dma((len(MOVES),)),
                dma((OWNERS,)),
                dma((OWNERS,)),
                dma((3, 4)),
                dma((3, 4)),
            ],
            compiler_params=pltpu.CompilerParams(
                collective_id=0, has_side_effects=True, vmem_limit_bytes=48 * 2**20
            ),
        )(master_down, router_weight.T, router_gain.reshape(1, width))
        final, router = pl.pallas_call(
            drain,
            out_shape=(
                jax.ShapeDtypeStruct(final.shape, final.dtype),
                jax.ShapeDtypeStruct(router.shape, router.dtype),
            ),
            in_specs=[pl.BlockSpec(memory_space=pl.ANY)] * 2,
            out_specs=(pl.BlockSpec(memory_space=pl.ANY), pl.BlockSpec(memory_space=pl.ANY)),
            scratch_shapes=[dma((17,))],
            compiler_params=pltpu.CompilerParams(vmem_limit_bytes=2**20),
        )(final, router)
        return jnp.swapaxes(final, 1, 2), router.T

    return jax.shard_map(
        shards,
        mesh=mesh,
        in_specs=(P("owner", None, "rows"), P("rows", "owner"), P("rows")),
        out_specs=(P("owner", None, "rows"), P()),
        check_vma=False,
    )
```

```python
import functools
import itertools

import jax
import jax.numpy as jnp
from jax import lax
from jax.experimental import pallas as pl
from jax.experimental.pallas import tpu as pltpu
from jax.sharding import PartitionSpec as P

MESH = pl.DeviceIdType.MESH
SIZES = (4, 4, 2)
ORDERS = ((0, 1, 2), (1, 2, 0), (2, 0, 1))
COLORS = range(3)
OWNERS = 4
STEPS = {2: (1,), 4: (1, 3, 2)}


def cuts_of(length, count, step):
    tiles = length // step
    edges = [tiles * k // count * step for k in range(count)] + [length]
    return [(a, b - a) for a, b in zip(edges, edges[1:])]


class Move:
    def __init__(self, color, phase, boxes, direct=False):
        self.color, self.phase, self.direct = color, phase, direct
        box = dict(zip(ORDERS[color], boxes))
        self.box = tuple(box[k] for k in range(3))
        self.dim = ORDERS[color][phase]
        self.step = self.box[self.dim][0]
        self.source = None if phase == 0 else 0 if phase == 1 or boxes[1] == (0, 1) else 1
        self.index = None

    def deltas(self):
        return list(itertools.product(*(range(a, a + n) for a, n in self.box)))

    def brought(self, delta):
        return max((q for q in range(self.phase) if delta[ORDERS[self.color][q]]), default=None)


def plan():
    zero = (0, 1)
    first, second, third, fourth = [], [], [], []
    for color in COLORS:
        na, nb, nc = (SIZES[d] for d in ORDERS[color])
        halves = [(0, nb // 2), (nb // 2, nb - nb // 2)] if na == 2 else [(0, nb)]
        first.append([Move(color, 0, ((a, 1), b, (0, nc))) for a in STEPS[na] for b in halves])
        second.append([Move(color, 1, (zero, (b, 1), (0, nc))) for b in STEPS[nb]])
        third.append([Move(color, 1, ((1, na - 1), (b, 1), (0, nc))) for b in STEPS[nb]])
        early = [Move(color, 2, ((0, na), zero, (c, 1))) for c in STEPS[nc]]
        groups = [(b, 1) for b in STEPS[nb]] if nc == 2 else [(1, nb - 1)]
        late = [((0, na), b, (c, 1)) for c in STEPS[nc] for b in groups]
        last = [
            Move(color, 2, ((a, 1), (b, 1), late[-1][2]), True)
            for b in range(late[-1][1][0], sum(late[-1][1]))
            for a in range(na)
        ]
        fourth.append((early, [Move(color, 2, boxes) for boxes in late[:-1]] + last))

    def woven(lists):
        return [m for row in itertools.zip_longest(*lists) for m in row if m is not None]

    stages = (
        woven(first),
        woven(second),
        woven(third),
        woven([early for early, _ in fourth]),
        woven([late for _, late in fourth]),
    )
    for k, m in enumerate(itertools.chain(*stages)):
        m.index = k
    return stages


STAGES = plan()
MOVES = list(itertools.chain(*STAGES))
BROUGHT = {(m.color, m.phase, d): m for m in MOVES for d in m.deltas()}
HEAD = 3


def kernel(cuts, x_ref, w_ref, g_ref, out_ref, router_ref, *scratch):
    loaded, held, *relays = (scratch[3 * k : 3 * k + 3] for k in range(5))
    parts, grid, load_sem, send_sem, recv_sem, part_send, part_recv, grid_send, grid_recv = scratch[15:]
    me = lax.axis_index("rows")
    own = lax.axis_index("owner")
    place = (me // 8, (me // 2) % 4, me % 2)
    depth = out_ref.shape[1]
    width = w_ref.shape[1]

    def moved(delta, sign=1):
        z, y, x = (lax.rem(p + sign * d + s, s) if d else p for p, d, s in zip(place, delta, SIZES))
        return (z * SIZES[1] + y) * SIZES[2] + x

    peers = {
        (dim, k): moved([k if d == dim else 0 for d in range(3)]) for dim in range(3) for k in range(1, SIZES[dim])
    }
    mates = [lax.rem(own + k, OWNERS) for k in range(OWNERS)]

    barrier = pltpu.get_barrier_semaphore()
    for peer in peers.values():
        pl.semaphore_signal(barrier, inc=1, device_id=(own, peer), device_id_type=MESH)
    for k in range(1, OWNERS):
        pl.semaphore_signal(barrier, inc=1, device_id=(mates[k], me), device_id_type=MESH)

    def load(color, delta):
        start, size = cuts[color]
        top = pl.multiple_of(moved(delta) * depth + start, 8)
        flat = (delta[0] * SIZES[1] + delta[1]) * SIZES[2] + delta[2]
        return pltpu.make_async_copy(
            x_ref.at[:, pl.ds(top, size), :], loaded[color].at[delta], load_sem.at[color, flat]
        )

    here = (0, 0, 0)
    for m in MOVES:
        for delta in m.deltas():
            if m.brought(delta) is None:
                load(m.color, delta).start()
    for color in COLORS:
        load(color, here).start()

    def column(delta):
        return pl.ds(pl.multiple_of(moved(delta, -1) * width, 128), width)

    def cast(m):
        target = held if m.source is None else relays[0]
        for delta in m.deltas():
            if m.brought(delta) is None:
                load(m.color, delta).wait()
                target[m.color][delta] = loaded[m.color][delta].astype(jnp.bfloat16)

    def copy(m):
        source = (held if m.source is None else relays[m.source])[m.color]
        target = relays[m.phase][m.color]
        if m.direct:
            (delta,) = m.deltas()
            start, size = cuts[m.color]
            dims = ORDERS[m.color]
            gone = tuple(0 if k == dims[2] else delta[k] for k in range(3))
            source, target = source.at[delta], out_ref.at[:, pl.ds(start, size), column(gone)]
        else:
            box = tuple(pl.ds(a, n) for a, n in m.box)
            source, target = source.at[box], target.at[box]
        return pltpu.make_async_remote_copy(
            src_ref=source,
            dst_ref=target,
            send_sem=send_sem.at[m.index],
            recv_sem=recv_sem.at[m.index],
            device_id=(own, peers[m.dim, m.step]),
            device_id_type=MESH,
        )

    arrived = set()

    def await_arrival(m):
        if m.index in arrived:
            return
        arrived.add(m.index)
        copy(m).wait_recv()
        if m.direct:
            return
        ended.extend((m, d) for d in m.deltas() if not any(d[ORDERS[m.color][q]] for q in range(m.phase + 1, 3)))

    ended = []

    def settle():
        for m, delta in ended:
            start, size = cuts[m.color]
            out_ref[:, pl.ds(start, size), column(delta)] = relays[m.phase][m.color][delta]
        ended.clear()

    def needs(m):
        came = {(m.brought(d), d) for d in m.deltas()}
        wanted = {BROUGHT[m.color, q, d].index for q, d in came if q is not None}
        return [MOVES[k] for k in sorted(wanted)]

    scaled = (w_ref[...] * g_ref[...]).astype(jnp.bfloat16).astype(jnp.float32)
    line = lax.broadcasted_iota(jnp.int32, (8, width), 0)
    pair = jnp.where(
        line % 2 == 0, jnp.broadcast_to(scaled[0:1, :], (8, width)), jnp.broadcast_to(scaled[1:2, :], (8, width))
    )
    parts[0] = pair.astype(jnp.bfloat16)

    def part_copy(k):
        return pltpu.make_async_remote_copy(
            src_ref=parts.at[0], dst_ref=parts.at[k], send_sem=part_send.at[k], recv_sem=part_recv.at[k],
            device_id=(mates[k], me), device_id_type=MESH)

    def grid_copies(dim):
        if dim == 0:
            block = grid.at[place[0], place[1], place[2]]
        elif dim == 1:
            block = grid.at[:, place[1], place[2]]
        else:
            block = grid.at[:, :, place[2]]
        return [
            pltpu.make_async_remote_copy(
                src_ref=block, dst_ref=block, send_sem=grid_send.at[dim, k], recv_sem=grid_recv.at[dim, k],
                device_id=(own, peers[dim, k]), device_id_type=MESH)
            for k in range(1, SIZES[dim])
        ]

    starts = STAGES[0]
    for m in starts[:HEAD]:
        cast(m)
    pl.semaphore_wait(barrier, len(peers) + OWNERS - 1)
    for k in range(1, OWNERS):
        part_copy(k).start()
    for m in starts[:HEAD]:
        copy(m).start()
    previous = None
    for m in starts[HEAD:]:
        cast(m)
        if previous is not None:
            copy(previous).start()
        previous = m
    for m in STAGES[1]:
        cast(m)
        if previous is not None:
            copy(previous).start()
        previous = m
    for m in STAGES[3]:
        cast(m)
    copy(previous).start()
    for color in COLORS:
        start, size = cuts[color]
        load(color, here).wait()
        out_ref[:, pl.ds(start, size), column(here)] = loaded[color][here].astype(jnp.bfloat16)

    for k, m in enumerate(STAGES[2]):
        for n in needs(m):
            await_arrival(n)
        copy(m).start()
        if k == 0:
            for j in range(1, OWNERS):
                part_copy(j).wait()
            tile = parts[0].astype(jnp.float32)
            for j in range(1, OWNERS):
                theirs = lax.rem(own - j + OWNERS, OWNERS)
                tile = jnp.where(line // 2 == theirs, parts[j].astype(jnp.float32), tile)
            grid[place[0], place[1], place[2]] = tile.astype(jnp.bfloat16)
        if k == 1:
            for c in grid_copies(0):
                c.start()
    for m in STAGES[3]:
        for n in needs(m):
            await_arrival(n)
        copy(m).start()
    for m in starts:
        await_arrival(m)
    settle()
    for c in grid_copies(0):
        c.wait()
    for c in grid_copies(1):
        c.start()
    for k, m in enumerate(STAGES[4]):
        for n in needs(m):
            await_arrival(n)
        copy(m).start()
        if k == 5:
            for c in grid_copies(1):
                c.wait()
            for c in grid_copies(2):
                c.start()
    settle()
    for m in MOVES[: len(STAGES[0]) + len(STAGES[1]) + len(STAGES[2])]:
        copy(m).wait_send()
    for c in grid_copies(2):
        c.wait()
    for row in range(32):
        router_ref[:, row * width : (row + 1) * width] = grid[row // 8, (row // 2) % 4, row % 2]
    for m in STAGES[3] + STAGES[4]:
        await_arrival(m)
        settle()
    for m in STAGES[3] + STAGES[4]:
        copy(m).wait_send()


def drain(final_ref, router_ref, final_out, router_out, sems):
    pieces = 8
    height = final_ref.shape[1] // pieces
    copies = [
        pltpu.make_async_copy(
            final_ref.at[e, pl.ds(k * height, height)], final_out.at[e, pl.ds(k * height, height)], sems.at[e * pieces + k]
        )
        for e in range(final_ref.shape[0])
        for k in range(pieces)
    ]
    copies.append(pltpu.make_async_copy(router_ref, router_out, sems.at[len(copies)]))
    for c in copies:
        c.start()
    for c in copies:
        c.wait()


def solution(mesh):
    def shards(master_down, router_weight, router_gain):
        experts, long, width = master_down.shape
        n = mesh.shape["rows"]
        depth = long // n
        cuts = cuts_of(depth, 3, 16)
        dma = pltpu.SemaphoreType.DMA
        blocks = [(*SIZES, experts, size, width) for _, size in cuts]
        final, router = pl.pallas_call(
            functools.partial(kernel, cuts),
            out_shape=(
                pltpu.VMEM((experts, depth, n * width), jnp.bfloat16),
                pltpu.VMEM((experts * OWNERS, n * width), jnp.bfloat16),
            ),
            in_specs=[
                pl.BlockSpec(memory_space=pl.ANY),
                pl.BlockSpec(memory_space=pltpu.VMEM),
                pl.BlockSpec(memory_space=pltpu.VMEM),
            ],
            out_specs=(pl.BlockSpec(memory_space=pltpu.VMEM), pl.BlockSpec(memory_space=pltpu.VMEM)),
            scratch_shapes=[pltpu.VMEM(b, jnp.float32) for b in blocks]
            + [pltpu.VMEM(b, jnp.bfloat16) for _ in range(4) for b in blocks]
            + [
                pltpu.VMEM((OWNERS, 8, width), jnp.bfloat16),
                pltpu.VMEM((*SIZES, 8, width), jnp.bfloat16),
                dma((3, n)),
                dma((len(MOVES),)),
                dma((len(MOVES),)),
                dma((OWNERS,)),
                dma((OWNERS,)),
                dma((3, 4)),
                dma((3, 4)),
            ],
            compiler_params=pltpu.CompilerParams(
                collective_id=0, has_side_effects=True, vmem_limit_bytes=48 * 2**20
            ),
        )(master_down, router_weight.T, router_gain.reshape(1, width))
        final, router = pl.pallas_call(
            drain,
            out_shape=(
                jax.ShapeDtypeStruct(final.shape, final.dtype),
                jax.ShapeDtypeStruct(router.shape, router.dtype),
            ),
            in_specs=[pl.BlockSpec(memory_space=pl.ANY)] * 2,
            out_specs=(pl.BlockSpec(memory_space=pl.ANY), pl.BlockSpec(memory_space=pl.ANY)),
            scratch_shapes=[dma((17,))],
            compiler_params=pltpu.CompilerParams(vmem_limit_bytes=2**20),
        )(final, router)
        return jnp.swapaxes(final, 1, 2), router.T

    return jax.shard_map(
        shards,
        mesh=mesh,
        in_specs=(P("owner", None, "rows"), P("rows", "owner"), P("rows")),
        out_specs=(P("owner", None, "rows"), P()),
        check_vma=False,
    )
```

```python
import functools
import itertools

import jax
import jax.numpy as jnp
from jax import lax
from jax.experimental import pallas as pl
from jax.experimental.pallas import tpu as pltpu
from jax.sharding import PartitionSpec as P

MESH = pl.DeviceIdType.MESH
SIZES = (4, 4, 2)
ORDERS = ((0, 1, 2), (1, 2, 0), (2, 0, 1))
COLORS = range(3)
OWNERS = 4
STEPS = {2: (1,), 4: (1, 3, 2)}


def cuts_of(length, count, step):
    tiles = length // step
    edges = [tiles * k // count * step for k in range(count)] + [length]
    return [(a, b - a) for a, b in zip(edges, edges[1:])]


class Move:
    def __init__(self, color, phase, boxes, direct=False):
        self.color, self.phase, self.direct = color, phase, direct
        box = dict(zip(ORDERS[color], boxes))
        self.box = tuple(box[k] for k in range(3))
        self.dim = ORDERS[color][phase]
        self.step = self.box[self.dim][0]
        self.source = None if phase == 0 else 0 if phase == 1 or boxes[1] == (0, 1) else 1
        self.index = None

    def deltas(self):
        return list(itertools.product(*(range(a, a + n) for a, n in self.box)))

    def brought(self, delta):
        return max((q for q in range(self.phase) if delta[ORDERS[self.color][q]]), default=None)


def plan():
    zero = (0, 1)
    first, second, third, fourth = [], [], [], []
    for color in COLORS:
        na, nb, nc = (SIZES[d] for d in ORDERS[color])
        halves = [(0, nb // 2), (nb // 2, nb - nb // 2)] if na == 2 else [(0, nb)]
        first.append([Move(color, 0, ((a, 1), b, (0, nc))) for a in STEPS[na] for b in halves])
        second.append([Move(color, 1, (zero, (b, 1), (0, nc))) for b in STEPS[nb]])
        third.append([Move(color, 1, ((1, na - 1), (b, 1), (0, nc))) for b in STEPS[nb]])
        early = [Move(color, 2, ((0, na), zero, (c, 1))) for c in STEPS[nc]]
        groups = [(b, 1) for b in STEPS[nb]] if nc == 2 else [(1, nb - 1)]
        late = [((0, na), b, (c, 1)) for c in STEPS[nc] for b in groups]
        last = [
            Move(color, 2, ((a, 1), (b, 1), late[-1][2]), True)
            for b in range(late[-1][1][0], sum(late[-1][1]))
            for a in range(na)
        ]
        fourth.append((early, [Move(color, 2, boxes) for boxes in late[:-1]] + last))

    def woven(lists):
        return [m for row in itertools.zip_longest(*lists) for m in row if m is not None]

    stages = (
        woven(first),
        woven(second),
        woven(third),
        woven([early for early, _ in fourth]),
        woven([late for _, late in fourth]),
    )
    for k, m in enumerate(itertools.chain(*stages)):
        m.index = k
    return stages


STAGES = plan()
MOVES = list(itertools.chain(*STAGES))
BROUGHT = {(m.color, m.phase, d): m for m in MOVES for d in m.deltas()}
HEAD = 3


def kernel(cuts, x_ref, w_ref, g_ref, out_ref, router_ref, *scratch):
    loaded, held, *relays = (scratch[3 * k : 3 * k + 3] for k in range(5))
    weight, gain, small_sem, parts, grid, load_sem, send_sem, recv_sem, part_send, part_recv, grid_send, grid_recv = scratch[15:]
    me = lax.axis_index("rows")
    own = lax.axis_index("owner")
    place = (me // 8, (me // 2) % 4, me % 2)
    depth = out_ref.shape[1]
    width = weight.shape[1]

    def moved(delta, sign=1):
        z, y, x = (lax.rem(p + sign * d + s, s) if d else p for p, d, s in zip(place, delta, SIZES))
        return (z * SIZES[1] + y) * SIZES[2] + x

    peers = {
        (dim, k): moved([k if d == dim else 0 for d in range(3)]) for dim in range(3) for k in range(1, SIZES[dim])
    }
    mates = [lax.rem(own + k, OWNERS) for k in range(OWNERS)]

    small = [
        pltpu.make_async_copy(w_ref, weight, small_sem.at[0]),
        pltpu.make_async_copy(g_ref, gain, small_sem.at[1]),
    ]
    for c in small:
        c.start()
    barrier = pltpu.get_barrier_semaphore()
    for peer in peers.values():
        pl.semaphore_signal(barrier, inc=1, device_id=(own, peer), device_id_type=MESH)
    for k in range(1, OWNERS):
        pl.semaphore_signal(barrier, inc=1, device_id=(mates[k], me), device_id_type=MESH)

    def load(color, delta):
        start, size = cuts[color]
        top = pl.multiple_of(moved(delta) * depth + start, 8)
        flat = (delta[0] * SIZES[1] + delta[1]) * SIZES[2] + delta[2]
        return pltpu.make_async_copy(
            x_ref.at[:, pl.ds(top, size), :], loaded[color].at[delta], load_sem.at[color, flat]
        )

    here = (0, 0, 0)
    for m in MOVES:
        for delta in m.deltas():
            if m.brought(delta) is None:
                load(m.color, delta).start()
    for color in COLORS:
        load(color, here).start()

    def column(delta):
        return pl.ds(pl.multiple_of(moved(delta, -1) * width, 128), width)

    def cast(m):
        target = held if m.source is None else relays[0]
        for delta in m.deltas():
            if m.brought(delta) is None:
                load(m.color, delta).wait()
                target[m.color][delta] = loaded[m.color][delta].astype(jnp.bfloat16)

    def copy(m):
        source = (held if m.source is None else relays[m.source])[m.color]
        target = relays[m.phase][m.color]
        if m.direct:
            (delta,) = m.deltas()
            start, size = cuts[m.color]
            dims = ORDERS[m.color]
            gone = tuple(0 if k == dims[2] else delta[k] for k in range(3))
            source, target = source.at[delta], out_ref.at[:, pl.ds(start, size), column(gone)]
        else:
            box = tuple(pl.ds(a, n) for a, n in m.box)
            source, target = source.at[box], target.at[box]
        return pltpu.make_async_remote_copy(
            src_ref=source,
            dst_ref=target,
            send_sem=send_sem.at[m.index],
            recv_sem=recv_sem.at[m.index],
            device_id=(own, peers[m.dim, m.step]),
            device_id_type=MESH,
        )

    arrived = set()

    def await_arrival(m):
        if m.index in arrived:
            return
        arrived.add(m.index)
        copy(m).wait_recv()
        if m.direct:
            return
        ended.extend((m, d) for d in m.deltas() if not any(d[ORDERS[m.color][q]] for q in range(m.phase + 1, 3)))

    ended = []

    def settle():
        for m, delta in ended:
            start, size = cuts[m.color]
            out_ref[:, pl.ds(start, size), column(delta)] = relays[m.phase][m.color][delta]
        ended.clear()

    def needs(m):
        came = {(m.brought(d), d) for d in m.deltas()}
        wanted = {BROUGHT[m.color, q, d].index for q, d in came if q is not None}
        return [MOVES[k] for k in sorted(wanted)]

    line = lax.broadcasted_iota(jnp.int32, (8, width), 0)

    def part_copy(k):
        return pltpu.make_async_remote_copy(
            src_ref=parts.at[0], dst_ref=parts.at[k], send_sem=part_send.at[k], recv_sem=part_recv.at[k],
            device_id=(mates[k], me), device_id_type=MESH)

    def grid_copies(dim):
        if dim == 0:
            block = grid.at[place[0], place[1], place[2]]
        elif dim == 1:
            block = grid.at[:, place[1], place[2]]
        else:
            block = grid.at[:, :, place[2]]
        return [
            pltpu.make_async_remote_copy(
                src_ref=block, dst_ref=block, send_sem=grid_send.at[dim, k], recv_sem=grid_recv.at[dim, k],
                device_id=(own, peers[dim, k]), device_id_type=MESH)
            for k in range(1, SIZES[dim])
        ]

    starts = STAGES[0]
    for m in starts[:HEAD]:
        cast(m)
    for c in small:
        c.wait()
    scaled = (weight[...] * gain[...]).astype(jnp.bfloat16).astype(jnp.float32)
    pair = jnp.where(
        line % 2 == 0, jnp.broadcast_to(scaled[0:1, :], (8, width)), jnp.broadcast_to(scaled[1:2, :], (8, width))
    )
    parts[0] = pair.astype(jnp.bfloat16)
    pl.semaphore_wait(barrier, len(peers) + OWNERS - 1)
    for k in range(1, OWNERS):
        part_copy(k).start()
    for m in starts[:HEAD]:
        copy(m).start()
    previous = None
    for m in starts[HEAD:]:
        cast(m)
        if previous is not None:
            copy(previous).start()
        previous = m
    for m in STAGES[1]:
        cast(m)
        if previous is not None:
            copy(previous).start()
        previous = m
    for m in STAGES[3]:
        cast(m)
    copy(previous).start()
    for color in COLORS:
        start, size = cuts[color]
        load(color, here).wait()
        out_ref[:, pl.ds(start, size), column(here)] = loaded[color][here].astype(jnp.bfloat16)

    for k, m in enumerate(STAGES[2]):
        for n in needs(m):
            await_arrival(n)
        copy(m).start()
        if k == 0:
            for j in range(1, OWNERS):
                part_copy(j).wait()
            tile = parts[0].astype(jnp.float32)
            for j in range(1, OWNERS):
                theirs = lax.rem(own - j + OWNERS, OWNERS)
                tile = jnp.where(line // 2 == theirs, parts[j].astype(jnp.float32), tile)
            grid[place[0], place[1], place[2]] = tile.astype(jnp.bfloat16)
        if k == 1:
            for c in grid_copies(0):
                c.start()
    for m in STAGES[3]:
        for n in needs(m):
            await_arrival(n)
        copy(m).start()
    for m in starts:
        await_arrival(m)
    settle()
    for c in grid_copies(0):
        c.wait()
    for c in grid_copies(1):
        c.start()
    for k, m in enumerate(STAGES[4]):
        for n in needs(m):
            await_arrival(n)
        copy(m).start()
        if k == 5:
            for c in grid_copies(1):
                c.wait()
            for c in grid_copies(2):
                c.start()
    settle()
    for m in MOVES[: len(STAGES[0]) + len(STAGES[1]) + len(STAGES[2])]:
        copy(m).wait_send()
    for c in grid_copies(2):
        c.wait()
    for row in range(32):
        router_ref[:, row * width : (row + 1) * width] = grid[row // 8, (row // 2) % 4, row % 2]
    for m in STAGES[3] + STAGES[4]:
        await_arrival(m)
        settle()
    for m in STAGES[3] + STAGES[4]:
        copy(m).wait_send()


def drain(final_ref, router_ref, final_out, router_out, sems):
    pieces = 8
    height = final_ref.shape[1] // pieces
    copies = [
        pltpu.make_async_copy(
            final_ref.at[e, pl.ds(k * height, height)], final_out.at[e, pl.ds(k * height, height)], sems.at[e * pieces + k]
        )
        for e in range(final_ref.shape[0])
        for k in range(pieces)
    ]
    copies.append(pltpu.make_async_copy(router_ref, router_out, sems.at[len(copies)]))
    for c in copies:
        c.start()
    for c in copies:
        c.wait()


def solution(mesh):
    def shards(master_down, router_weight, router_gain):
        experts, long, width = master_down.shape
        n = mesh.shape["rows"]
        depth = long // n
        cuts = cuts_of(depth, 3, 8)
        dma = pltpu.SemaphoreType.DMA
        blocks = [(*SIZES, experts, size, width) for _, size in cuts]
        final, router = pl.pallas_call(
            functools.partial(kernel, cuts),
            out_shape=(
                pltpu.VMEM((experts, depth, n * width), jnp.bfloat16),
                pltpu.VMEM((experts * OWNERS, n * width), jnp.bfloat16),
            ),
            in_specs=[pl.BlockSpec(memory_space=pl.ANY)] * 3,
            out_specs=(pl.BlockSpec(memory_space=pltpu.VMEM), pl.BlockSpec(memory_space=pltpu.VMEM)),
            scratch_shapes=[pltpu.VMEM(b, jnp.float32) for b in blocks]
            + [pltpu.VMEM(b, jnp.bfloat16) for _ in range(4) for b in blocks]
            + [
                pltpu.VMEM((2, width), jnp.float32),
                pltpu.VMEM((1, width), jnp.float32),
                dma((2,)),
                pltpu.VMEM((OWNERS, 8, width), jnp.bfloat16),
                pltpu.VMEM((*SIZES, 8, width), jnp.bfloat16),
                dma((3, n)),
                dma((len(MOVES),)),
                dma((len(MOVES),)),
                dma((OWNERS,)),
                dma((OWNERS,)),
                dma((3, 4)),
                dma((3, 4)),
            ],
            compiler_params=pltpu.CompilerParams(
                collective_id=0, has_side_effects=True, vmem_limit_bytes=48 * 2**20
            ),
        )(master_down, router_weight.T, router_gain.reshape(1, width))
        final, router = pl.pallas_call(
            drain,
            out_shape=(
                jax.ShapeDtypeStruct(final.shape, final.dtype),
                jax.ShapeDtypeStruct(router.shape, router.dtype),
            ),
            in_specs=[pl.BlockSpec(memory_space=pl.ANY)] * 2,
            out_specs=(pl.BlockSpec(memory_space=pl.ANY), pl.BlockSpec(memory_space=pl.ANY)),
            scratch_shapes=[dma((17,))],
            compiler_params=pltpu.CompilerParams(vmem_limit_bytes=2**20),
        )(final, router)
        return jnp.swapaxes(final, 1, 2), router.T

    return jax.shard_map(
        shards,
        mesh=mesh,
        in_specs=(P("owner", None, "rows"), P("rows", "owner"), P("rows")),
        out_specs=(P("owner", None, "rows"), P()),
        check_vma=False,
    )
```

```python
import functools
import itertools

import jax
import jax.numpy as jnp
from jax import lax
from jax.experimental import pallas as pl
from jax.experimental.pallas import tpu as pltpu
from jax.sharding import PartitionSpec as P

MESH = pl.DeviceIdType.MESH
SIZES = (4, 4, 2)
ORDERS = ((0, 1, 2), (1, 2, 0), (2, 0, 1))
COLORS = range(3)
OWNERS = 4
STEPS = {2: (1,), 4: (1, 3, 2)}


def cuts_of(length, count, step):
    tiles = length // step
    edges = [tiles * k // count * step for k in range(count)] + [length]
    return [(a, b - a) for a, b in zip(edges, edges[1:])]


class Move:
    def __init__(self, color, phase, boxes, direct=False):
        self.color, self.phase, self.direct = color, phase, direct
        box = dict(zip(ORDERS[color], boxes))
        self.box = tuple(box[k] for k in range(3))
        self.dim = ORDERS[color][phase]
        self.step = self.box[self.dim][0]
        self.source = None if phase == 0 else 0 if phase == 1 or boxes[1] == (0, 1) else 1
        self.index = None

    def deltas(self):
        return list(itertools.product(*(range(a, a + n) for a, n in self.box)))

    def brought(self, delta):
        return max((q for q in range(self.phase) if delta[ORDERS[self.color][q]]), default=None)


def plan():
    zero = (0, 1)
    first, second, third, fourth = [], [], [], []
    for color in COLORS:
        na, nb, nc = (SIZES[d] for d in ORDERS[color])
        halves = [(0, nb // 2), (nb // 2, nb - nb // 2)] if na == 2 else [(0, nb)]
        first.append([Move(color, 0, ((a, 1), b, (0, nc))) for a in STEPS[na] for b in halves])
        second.append([Move(color, 1, (zero, (b, 1), (0, nc))) for b in STEPS[nb]])
        third.append([Move(color, 1, (a, (b, 1), (0, nc))) for a in ([(k, 1) for k in STEPS[na]] if nb == 2 else [(1, na - 1)]) for b in STEPS[nb]])
        early = [Move(color, 2, ((0, na), zero, (c, 1))) for c in STEPS[nc]]
        groups = [(b, 1) for b in STEPS[nb]] if nc == 2 else [(1, nb - 1)]
        late = [((0, na), b, (c, 1)) for c in STEPS[nc] for b in groups]
        last = [
            Move(color, 2, ((a, 1), (b, 1), late[-1][2]), True)
            for b in range(late[-1][1][0], sum(late[-1][1]))
            for a in range(na)
        ]
        fourth.append((early, [Move(color, 2, boxes) for boxes in late[:-1]] + last))

    def woven(lists):
        return [m for row in itertools.zip_longest(*lists) for m in row if m is not None]

    stages = (
        woven(first),
        woven(second),
        woven(third),
        woven([early for early, _ in fourth]),
        woven([late for _, late in fourth]),
    )
    for k, m in enumerate(itertools.chain(*stages)):
        m.index = k
    return stages


STAGES = plan()
MOVES = list(itertools.chain(*STAGES))
BROUGHT = {(m.color, m.phase, d): m for m in MOVES for d in m.deltas()}
HEAD = 3


def kernel(cuts, x_ref, w_ref, g_ref, out_ref, router_ref, *scratch):
    loaded, held, *relays = (scratch[3 * k : 3 * k + 3] for k in range(5))
    weight, gain, small_sem, parts, grid, load_sem, send_sem, recv_sem, part_send, part_recv, grid_send, grid_recv = scratch[15:]
    me = lax.axis_index("rows")
    own = lax.axis_index("owner")
    place = (me // 8, (me // 2) % 4, me % 2)
    depth = out_ref.shape[1]
    width = weight.shape[1]

    def moved(delta, sign=1):
        z, y, x = (lax.rem(p + sign * d + s, s) if d else p for p, d, s in zip(place, delta, SIZES))
        return (z * SIZES[1] + y) * SIZES[2] + x

    peers = {
        (dim, k): moved([k if d == dim else 0 for d in range(3)]) for dim in range(3) for k in range(1, SIZES[dim])
    }
    mates = [lax.rem(own + k, OWNERS) for k in range(OWNERS)]

    small = [
        pltpu.make_async_copy(w_ref, weight, small_sem.at[0]),
        pltpu.make_async_copy(g_ref, gain, small_sem.at[1]),
    ]
    for c in small:
        c.start()
    barrier = pltpu.get_barrier_semaphore()
    for peer in peers.values():
        pl.semaphore_signal(barrier, inc=1, device_id=(own, peer), device_id_type=MESH)
    for k in range(1, OWNERS):
        pl.semaphore_signal(barrier, inc=1, device_id=(mates[k], me), device_id_type=MESH)

    def load(color, delta):
        start, size = cuts[color]
        top = pl.multiple_of(moved(delta) * depth + start, 8)
        flat = (delta[0] * SIZES[1] + delta[1]) * SIZES[2] + delta[2]
        return pltpu.make_async_copy(
            x_ref.at[:, pl.ds(top, size), :], loaded[color].at[delta], load_sem.at[color, flat]
        )

    here = (0, 0, 0)
    for m in MOVES:
        for delta in m.deltas():
            if m.brought(delta) is None:
                load(m.color, delta).start()
    for color in COLORS:
        load(color, here).start()

    def column(delta):
        return pl.ds(pl.multiple_of(moved(delta, -1) * width, 128), width)

    def cast(m):
        target = held if m.source is None else relays[0]
        for delta in m.deltas():
            if m.brought(delta) is None:
                load(m.color, delta).wait()
                target[m.color][delta] = loaded[m.color][delta].astype(jnp.bfloat16)

    def copy(m):
        source = (held if m.source is None else relays[m.source])[m.color]
        target = relays[m.phase][m.color]
        if m.direct:
            (delta,) = m.deltas()
            start, size = cuts[m.color]
            dims = ORDERS[m.color]
            gone = tuple(0 if k == dims[2] else delta[k] for k in range(3))
            source, target = source.at[delta], out_ref.at[:, pl.ds(start, size), column(gone)]
        else:
            box = tuple(pl.ds(a, n) for a, n in m.box)
            source, target = source.at[box], target.at[box]
        return pltpu.make_async_remote_copy(
            src_ref=source,
            dst_ref=target,
            send_sem=send_sem.at[m.index],
            recv_sem=recv_sem.at[m.index],
            device_id=(own, peers[m.dim, m.step]),
            device_id_type=MESH,
        )

    arrived = set()

    def await_arrival(m):
        if m.index in arrived:
            return
        arrived.add(m.index)
        copy(m).wait_recv()
        if m.direct:
            return
        ended.extend((m, d) for d in m.deltas() if not any(d[ORDERS[m.color][q]] for q in range(m.phase + 1, 3)))

    ended = []

    def settle():
        for m, delta in ended:
            start, size = cuts[m.color]
            out_ref[:, pl.ds(start, size), column(delta)] = relays[m.phase][m.color][delta]
        ended.clear()

    def needs(m):
        came = {(m.brought(d), d) for d in m.deltas()}
        wanted = {BROUGHT[m.color, q, d].index for q, d in came if q is not None}
        return [MOVES[k] for k in sorted(wanted)]

    line = lax.broadcasted_iota(jnp.int32, (8, width), 0)

    def part_copy(k):
        return pltpu.make_async_remote_copy(
            src_ref=parts.at[0], dst_ref=parts.at[k], send_sem=part_send.at[k], recv_sem=part_recv.at[k],
            device_id=(mates[k], me), device_id_type=MESH)

    def grid_copies(dim):
        if dim == 0:
            block = grid.at[place[0], place[1], place[2]]
        elif dim == 1:
            block = grid.at[:, place[1], place[2]]
        else:
            block = grid.at[:, :, place[2]]
        return [
            pltpu.make_async_remote_copy(
                src_ref=block, dst_ref=block, send_sem=grid_send.at[dim, k], recv_sem=grid_recv.at[dim, k],
                device_id=(own, peers[dim, k]), device_id_type=MESH)
            for k in range(1, SIZES[dim])
        ]

    starts = STAGES[0]
    cast(starts[0])
    for c in small:
        c.wait()
    scaled = (weight[...] * gain[...]).astype(jnp.bfloat16).astype(jnp.float32)
    pair = jnp.where(
        line % 2 == 0, jnp.broadcast_to(scaled[0:1, :], (8, width)), jnp.broadcast_to(scaled[1:2, :], (8, width))
    )
    parts[0] = pair.astype(jnp.bfloat16)
    for m in starts[1:HEAD]:
        cast(m)
    pl.semaphore_wait(barrier, len(peers) + OWNERS - 1)
    for k in range(1, OWNERS):
        part_copy(k).start()
    for m in starts[:HEAD]:
        copy(m).start()
    previous = None
    for m in starts[HEAD:]:
        cast(m)
        if previous is not None:
            copy(previous).start()
        previous = m
    for m in STAGES[1]:
        cast(m)
        if previous is not None:
            copy(previous).start()
        previous = m
    for m in STAGES[3]:
        cast(m)
    copy(previous).start()
    for color in COLORS:
        start, size = cuts[color]
        load(color, here).wait()
        out_ref[:, pl.ds(start, size), column(here)] = loaded[color][here].astype(jnp.bfloat16)

    for k, m in enumerate(STAGES[2]):
        for n in needs(m):
            await_arrival(n)
        copy(m).start()
        if k == 0:
            for j in range(1, OWNERS):
                part_copy(j).wait()
            tile = parts[0].astype(jnp.float32)
            for j in range(1, OWNERS):
                theirs = lax.rem(own - j + OWNERS, OWNERS)
                tile = jnp.where(line // 2 == theirs, parts[j].astype(jnp.float32), tile)
            grid[place[0], place[1], place[2]] = tile.astype(jnp.bfloat16)
        if k == 1:
            for c in grid_copies(0):
                c.start()
    for m in STAGES[3]:
        for n in needs(m):
            await_arrival(n)
        copy(m).start()
    for m in starts:
        await_arrival(m)
    settle()
    for c in grid_copies(0):
        c.wait()
    for c in grid_copies(1):
        c.start()
    for k, m in enumerate(STAGES[4]):
        for n in needs(m):
            await_arrival(n)
        copy(m).start()
        if k == 5:
            for c in grid_copies(1):
                c.wait()
            for c in grid_copies(2):
                c.start()
    settle()
    for m in MOVES[: len(STAGES[0]) + len(STAGES[1]) + len(STAGES[2])]:
        copy(m).wait_send()
    for c in grid_copies(2):
        c.wait()
    for row in range(32):
        router_ref[:, row * width : (row + 1) * width] = grid[row // 8, (row // 2) % 4, row % 2]
    for m in STAGES[3] + STAGES[4]:
        await_arrival(m)
        settle()
    for m in STAGES[3] + STAGES[4]:
        copy(m).wait_send()


def drain(final_ref, router_ref, final_out, router_out, sems):
    pieces = 8
    height = final_ref.shape[1] // pieces
    copies = [
        pltpu.make_async_copy(
            final_ref.at[e, pl.ds(k * height, height)], final_out.at[e, pl.ds(k * height, height)], sems.at[e * pieces + k]
        )
        for e in range(final_ref.shape[0])
        for k in range(pieces)
    ]
    copies.append(pltpu.make_async_copy(router_ref, router_out, sems.at[len(copies)]))
    for c in copies:
        c.start()
    for c in copies:
        c.wait()


def solution(mesh):
    def shards(master_down, router_weight, router_gain):
        experts, long, width = master_down.shape
        n = mesh.shape["rows"]
        depth = long // n
        cuts = cuts_of(depth, 3, 8)
        dma = pltpu.SemaphoreType.DMA
        blocks = [(*SIZES, experts, size, width) for _, size in cuts]
        final, router = pl.pallas_call(
            functools.partial(kernel, cuts),
            out_shape=(
                pltpu.VMEM((experts, depth, n * width), jnp.bfloat16),
                pltpu.VMEM((experts * OWNERS, n * width), jnp.bfloat16),
            ),
            in_specs=[pl.BlockSpec(memory_space=pl.ANY)] * 3,
            out_specs=(pl.BlockSpec(memory_space=pltpu.VMEM), pl.BlockSpec(memory_space=pltpu.VMEM)),
            scratch_shapes=[pltpu.VMEM(b, jnp.float32) for b in blocks]
            + [pltpu.VMEM(b, jnp.bfloat16) for _ in range(4) for b in blocks]
            + [
                pltpu.VMEM((2, width), jnp.float32),
                pltpu.VMEM((1, width), jnp.float32),
                dma((2,)),
                pltpu.VMEM((OWNERS, 8, width), jnp.bfloat16),
                pltpu.VMEM((*SIZES, 8, width), jnp.bfloat16),
                dma((3, n)),
                dma((len(MOVES),)),
                dma((len(MOVES),)),
                dma((OWNERS,)),
                dma((OWNERS,)),
                dma((3, 4)),
                dma((3, 4)),
            ],
            compiler_params=pltpu.CompilerParams(
                collective_id=0, has_side_effects=True, vmem_limit_bytes=48 * 2**20
            ),
        )(master_down, router_weight.T, router_gain.reshape(1, width))
        final, router = pl.pallas_call(
            drain,
            out_shape=(
                jax.ShapeDtypeStruct(final.shape, final.dtype),
                jax.ShapeDtypeStruct(router.shape, router.dtype),
            ),
            in_specs=[pl.BlockSpec(memory_space=pl.ANY)] * 2,
            out_specs=(pl.BlockSpec(memory_space=pl.ANY), pl.BlockSpec(memory_space=pl.ANY)),
            scratch_shapes=[dma((17,))],
            compiler_params=pltpu.CompilerParams(vmem_limit_bytes=2**20),
        )(final, router)
        return jnp.swapaxes(final, 1, 2), router.T

    return jax.shard_map(
        shards,
        mesh=mesh,
        in_specs=(P("owner", None, "rows"), P("rows", "owner"), P("rows")),
        out_specs=(P("owner", None, "rows"), P()),
        check_vma=False,
    )
```

```python
import functools
import itertools

import jax
import jax.numpy as jnp
from jax import lax
from jax.experimental import pallas as pl
from jax.experimental.pallas import tpu as pltpu
from jax.sharding import PartitionSpec as P

MESH = pl.DeviceIdType.MESH
SIZES = (4, 4, 2)
ORDERS = ((0, 1, 2), (1, 2, 0), (2, 0, 1))
COLORS = range(3)
OWNERS = 4
STEPS = {2: (1,), 4: (1, 3, 2)}


def cuts_of(length, count, step):
    tiles = length // step
    edges = [tiles * k // count * step for k in range(count)] + [length]
    return [(a, b - a) for a, b in zip(edges, edges[1:])]


class Move:
    def __init__(self, color, phase, boxes, direct=False):
        self.color, self.phase, self.direct = color, phase, direct
        box = dict(zip(ORDERS[color], boxes))
        self.box = tuple(box[k] for k in range(3))
        self.dim = ORDERS[color][phase]
        self.step = self.box[self.dim][0]
        self.source = None if phase == 0 else 0 if phase == 1 or boxes[1] == (0, 1) else 1
        self.index = None

    def deltas(self):
        return list(itertools.product(*(range(a, a + n) for a, n in self.box)))

    def brought(self, delta):
        return max((q for q in range(self.phase) if delta[ORDERS[self.color][q]]), default=None)


def plan():
    zero = (0, 1)
    first, second, third, fourth = [], [], [], []
    for color in COLORS:
        na, nb, nc = (SIZES[d] for d in ORDERS[color])
        halves = [(0, nb // 2), (nb // 2, nb - nb // 2)] if na == 2 else [(0, nb)]
        first.append([Move(color, 0, ((a, 1), b, (0, nc))) for a in STEPS[na] for b in halves])
        second.append([Move(color, 1, (zero, (b, 1), (0, nc))) for b in STEPS[nb]])
        third.append([Move(color, 1, ((1, na - 1), (b, 1), (0, nc))) for b in STEPS[nb]])
        early = [Move(color, 2, ((0, na), zero, (c, 1))) for c in STEPS[nc]]
        groups = [(b, 1) for b in STEPS[nb]] if nc == 2 else [(1, nb - 1)]
        late = [((0, na), b, (c, 1)) for c in STEPS[nc] for b in groups]
        last = [
            Move(color, 2, ((a, 1), (b, 1), late[-1][2]), True)
            for b in range(late[-1][1][0], sum(late[-1][1]))
            for a in range(na)
        ]
        fourth.append((early, [Move(color, 2, boxes) for boxes in late[:-1]] + last))

    def woven(lists):
        return [m for row in itertools.zip_longest(*lists) for m in row if m is not None]

    stages = (
        woven(first),
        woven(second),
        woven(third),
        woven([early for early, _ in fourth]),
        woven([late for _, late in fourth]),
    )
    for k, m in enumerate(itertools.chain(*stages)):
        m.index = k
    return stages


STAGES = plan()
MOVES = list(itertools.chain(*STAGES))
BROUGHT = {(m.color, m.phase, d): m for m in MOVES for d in m.deltas()}
HEAD = 3


def kernel(cuts, x_ref, w_ref, g_ref, out_ref, router_ref, *scratch):
    loaded, held, *relays = (scratch[3 * k : 3 * k + 3] for k in range(5))
    weight, gain, small_sem, parts, grid, load_sem, send_sem, recv_sem, part_send, part_recv, grid_send, grid_recv = scratch[15:]
    me = lax.axis_index("rows")
    own = lax.axis_index("owner")
    place = (me // 8, (me // 2) % 4, me % 2)
    depth = out_ref.shape[1]
    width = weight.shape[1]

    def moved(delta, sign=1):
        z, y, x = (lax.rem(p + sign * d + s, s) if d else p for p, d, s in zip(place, delta, SIZES))
        return (z * SIZES[1] + y) * SIZES[2] + x

    peers = {
        (dim, k): moved([k if d == dim else 0 for d in range(3)]) for dim in range(3) for k in range(1, SIZES[dim])
    }
    mates = [lax.rem(own + k, OWNERS) for k in range(OWNERS)]

    small = [
        pltpu.make_async_copy(w_ref, weight, small_sem.at[0]),
        pltpu.make_async_copy(g_ref, gain, small_sem.at[1]),
    ]
    for c in small:
        c.start()
    barrier = pltpu.get_barrier_semaphore()
    for peer in [peers[d, SIZES[d] // 2] for d in (2, 1, 0)] + [peers[d, k] for d in (0, 1) for k in (1, 3)]:
        pl.semaphore_signal(barrier, inc=1, device_id=(own, peer), device_id_type=MESH)
    for k in range(1, OWNERS):
        pl.semaphore_signal(barrier, inc=1, device_id=(mates[k], me), device_id_type=MESH)

    def load(color, delta):
        start, size = cuts[color]
        top = pl.multiple_of(moved(delta) * depth + start, 8)
        flat = (delta[0] * SIZES[1] + delta[1]) * SIZES[2] + delta[2]
        return pltpu.make_async_copy(
            x_ref.at[:, pl.ds(top, size), :], loaded[color].at[delta], load_sem.at[color, flat]
        )

    here = (0, 0, 0)
    for m in MOVES:
        for delta in m.deltas():
            if m.brought(delta) is None:
                load(m.color, delta).start()
    for color in COLORS:
        load(color, here).start()

    def column(delta):
        return pl.ds(pl.multiple_of(moved(delta, -1) * width, 128), width)

    def cast(m):
        target = held if m.source is None else relays[0]
        for delta in m.deltas():
            if m.brought(delta) is None:
                load(m.color, delta).wait()
                target[m.color][delta] = loaded[m.color][delta].astype(jnp.bfloat16)

    def copy(m):
        source = (held if m.source is None else relays[m.source])[m.color]
        target = relays[m.phase][m.color]
        if m.direct:
            (delta,) = m.deltas()
            start, size = cuts[m.color]
            dims = ORDERS[m.color]
            gone = tuple(0 if k == dims[2] else delta[k] for k in range(3))
            source, target = source.at[delta], out_ref.at[:, pl.ds(start, size), column(gone)]
        else:
            box = tuple(pl.ds(a, n) for a, n in m.box)
            source, target = source.at[box], target.at[box]
        return pltpu.make_async_remote_copy(
            src_ref=source,
            dst_ref=target,
            send_sem=send_sem.at[m.index],
            recv_sem=recv_sem.at[m.index],
            device_id=(own, peers[m.dim, m.step]),
            device_id_type=MESH,
        )

    arrived = set()

    def await_arrival(m):
        if m.index in arrived:
            return
        arrived.add(m.index)
        copy(m).wait_recv()
        if m.direct:
            return
        ended.extend((m, d) for d in m.deltas() if not any(d[ORDERS[m.color][q]] for q in range(m.phase + 1, 3)))

    ended = []

    def settle():
        for m, delta in ended:
            start, size = cuts[m.color]
            out_ref[:, pl.ds(start, size), column(delta)] = relays[m.phase][m.color][delta]
        ended.clear()

    def needs(m):
        came = {(m.brought(d), d) for d in m.deltas()}
        wanted = {BROUGHT[m.color, q, d].index for q, d in came if q is not None}
        return [MOVES[k] for k in sorted(wanted)]

    line = lax.broadcasted_iota(jnp.int32, (8, width), 0)

    def part_copy(k):
        return pltpu.make_async_remote_copy(
            src_ref=parts.at[0], dst_ref=parts.at[k], send_sem=part_send.at[k], recv_sem=part_recv.at[k],
            device_id=(mates[k], me), device_id_type=MESH)

    def grid_copies(dim):
        if dim == 2:
            block = grid.at[place[0], place[1], place[2]]
        elif dim == 0:
            block = grid.at[place[0], place[1]]
        else:
            block = grid.at[:, place[1]]
        return [
            pltpu.make_async_remote_copy(
                src_ref=block, dst_ref=block, send_sem=grid_send.at[dim, k], recv_sem=grid_recv.at[dim, k],
                device_id=(own, peers[dim, k]), device_id_type=MESH)
            for k in range(1, SIZES[dim])
        ]

    starts = STAGES[0]
    for m in starts[:HEAD]:
        cast(m)
    for c in small:
        c.wait()
    scaled = (weight[...] * gain[...]).astype(jnp.bfloat16).astype(jnp.float32)
    pair = jnp.where(
        line % 2 == 0, jnp.broadcast_to(scaled[0:1, :], (8, width)), jnp.broadcast_to(scaled[1:2, :], (8, width))
    )
    parts[0] = pair.astype(jnp.bfloat16)
    pl.semaphore_wait(barrier, len(peers) + OWNERS - 1)
    for k in range(1, OWNERS):
        part_copy(k).start()
    for m in starts[:HEAD]:
        copy(m).start()
    previous = None
    for m in starts[HEAD:]:
        cast(m)
        if previous is not None:
            copy(previous).start()
        previous = m
    for m in STAGES[1]:
        cast(m)
        if previous is not None:
            copy(previous).start()
        previous = m
    for m in STAGES[3]:
        cast(m)
    copy(previous).start()
    for color in COLORS:
        start, size = cuts[color]
        load(color, here).wait()
        out_ref[:, pl.ds(start, size), column(here)] = loaded[color][here].astype(jnp.bfloat16)

    for k, m in enumerate(STAGES[2]):
        for n in needs(m):
            await_arrival(n)
        copy(m).start()
        if k == 0:
            for j in range(1, OWNERS):
                part_copy(j).wait()
            tile = parts[0].astype(jnp.float32)
            for j in range(1, OWNERS):
                theirs = lax.rem(own - j + OWNERS, OWNERS)
                tile = jnp.where(line // 2 == theirs, parts[j].astype(jnp.float32), tile)
            grid[place[0], place[1], place[2]] = tile.astype(jnp.bfloat16)
        if k == 1:
            for c in grid_copies(2):
                c.start()
    for m in STAGES[3]:
        for n in needs(m):
            await_arrival(n)
        copy(m).start()
    for m in starts:
        await_arrival(m)
    settle()
    for c in grid_copies(2):
        c.wait()
    for c in grid_copies(0):
        c.start()
    for k, m in enumerate(STAGES[4]):
        for n in needs(m):
            await_arrival(n)
        copy(m).start()
        if k == 5:
            for c in grid_copies(0):
                c.wait()
            for c in grid_copies(1):
                c.start()
    settle()
    for m in MOVES[: len(STAGES[0]) + len(STAGES[1]) + len(STAGES[2])]:
        copy(m).wait_send()
    for c in grid_copies(1):
        c.wait()
    for row in range(32):
        router_ref[:, row * width : (row + 1) * width] = grid[row // 8, (row // 2) % 4, row % 2]
    for m in STAGES[3] + STAGES[4]:
        await_arrival(m)
        settle()
        copy(m).wait_send()


def drain(final_ref, router_ref, final_out, router_out, sems):
    pieces = 8
    height = final_ref.shape[1] // pieces
    copies = [
        pltpu.make_async_copy(
            final_ref.at[e, pl.ds(k * height, height)], final_out.at[e, pl.ds(k * height, height)], sems.at[e * pieces + k]
        )
        for e in range(final_ref.shape[0])
        for k in range(pieces)
    ]
    copies.append(pltpu.make_async_copy(router_ref, router_out, sems.at[len(copies)]))
    for c in copies:
        c.start()
    for c in copies:
        c.wait()


def solution(mesh):
    def shards(master_down, router_weight, router_gain):
        experts, long, width = master_down.shape
        n = mesh.shape["rows"]
        depth = long // n
        cuts = cuts_of(depth, 3, 8)
        dma = pltpu.SemaphoreType.DMA
        blocks = [(*SIZES, experts, size, width) for _, size in cuts]
        final, router = pl.pallas_call(
            functools.partial(kernel, cuts),
            out_shape=(
                pltpu.VMEM((experts, depth, n * width), jnp.bfloat16),
                pltpu.VMEM((experts * OWNERS, n * width), jnp.bfloat16),
            ),
            in_specs=[pl.BlockSpec(memory_space=pl.ANY)] * 3,
            out_specs=(pl.BlockSpec(memory_space=pltpu.VMEM), pl.BlockSpec(memory_space=pltpu.VMEM)),
            scratch_shapes=[pltpu.VMEM(b, jnp.float32) for b in blocks]
            + [pltpu.VMEM(b, jnp.bfloat16) for _ in range(4) for b in blocks]
            + [
                pltpu.VMEM((2, width), jnp.float32),
                pltpu.VMEM((1, width), jnp.float32),
                dma((2,)),
                pltpu.VMEM((OWNERS, 8, width), jnp.bfloat16),
                pltpu.VMEM((*SIZES, 8, width), jnp.bfloat16),
                dma((3, n)),
                dma((len(MOVES),)),
                dma((len(MOVES),)),
                dma((OWNERS,)),
                dma((OWNERS,)),
                dma((3, 4)),
                dma((3, 4)),
            ],
            compiler_params=pltpu.CompilerParams(
                collective_id=0, has_side_effects=True, vmem_limit_bytes=48 * 2**20
            ),
        )(master_down, router_weight.T, router_gain.reshape(1, width))
        final, router = pl.pallas_call(
            drain,
            out_shape=(
                jax.ShapeDtypeStruct(final.shape, final.dtype),
                jax.ShapeDtypeStruct(router.shape, router.dtype),
            ),
            in_specs=[pl.BlockSpec(memory_space=pl.ANY)] * 2,
            out_specs=(pl.BlockSpec(memory_space=pl.ANY), pl.BlockSpec(memory_space=pl.ANY)),
            scratch_shapes=[dma((17,))],
            compiler_params=pltpu.CompilerParams(vmem_limit_bytes=2**20),
        )(final, router)
        return jnp.swapaxes(final, 1, 2), router.T

    return jax.shard_map(
        shards,
        mesh=mesh,
        in_specs=(P("owner", None, "rows"), P("rows", "owner"), P("rows")),
        out_specs=(P("owner", None, "rows"), P()),
        check_vma=False,
    )
```
